8 devices in a mesh: tp: 8 (over z, y, x, core).
Axes of the slice: x: 2, y: 2, z: 1, core: 2. Of those that a mesh axis runs over, the one named last changes fastest.
Arguments:
- hidden: bfloat16 [3, 4096, 4096], P(None, 'tp')
- labels: int32 [3, 4096], P(None, 'tp')
- loss_mask: int32 [3, 4096], P(None, 'tp')
- norm_gain: float32 [4096], replicated
- w_head: bfloat16 [4096, 32768], P(None, 'tp')
Outputs:
- output 1: float32 [], replicated
- output 2: bfloat16 [3, 4096, 4096], P(None, 'tp')
- output 3: bfloat16 [4096, 32768], P(None, 'tp')
- output 4: float32 [4096], replicated
All inputs are finite; a program needn't handle non-finite values.
Results may differ from the reference program's by a relative error of at most 0.00838527.
Values are sent between devices in bfloat16 or wider.
A program may use at most 1 GiB of HBM per device.

```python
import jax
import jax.numpy as jnp
from jax import lax

BATCH_SIZE = 3
SEQ_DEV = 512
D_MODEL = 4096
VOCAB_SIZE = 32768
SHARDS = 8
SEQ_LEN = SEQ_DEV * SHARDS
VSHARD = VOCAB_SIZE // SHARDS
NORM_EPS = 1e-6
LOGIT_STD = 3.0
LABEL_PULL = 2.0


def draw_targets(route_key):
    key_hot, key_pick, key_uni, key_loc, key_rate, key_keep = jax.random.split(route_key, 6)
    hot_block = jax.random.randint(key_hot, (), 0, SHARDS)
    use_hot = jax.random.randint(key_pick, (BATCH_SIZE, SEQ_LEN), 0, 2)
    spread_ids = jax.random.randint(key_uni, (BATCH_SIZE, SEQ_LEN), 0, VOCAB_SIZE)
    hot_ids = hot_block * VSHARD + jax.random.randint(key_loc, (BATCH_SIZE, SEQ_LEN), 0, VSHARD)
    labels = jnp.where(use_hot == 1, hot_ids, spread_ids).astype(jnp.int32)
    keep_rate = jax.random.randint(key_rate, (BATCH_SIZE, SHARDS, 1), 1, 9)
    keep_draw = jax.random.randint(key_keep, (BATCH_SIZE, SHARDS, SEQ_DEV), 0, 8)
    loss_mask = (keep_draw < keep_rate).astype(jnp.int32).reshape(BATCH_SIZE, SEQ_LEN)
    first_pos = (jnp.arange(SEQ_LEN) == 0).astype(jnp.int32)
    loss_mask = jnp.maximum(loss_mask, first_pos[None, :])
    return labels, loss_mask


def setup_inputs(seed: int = 0) -> dict:
    root_key = jax.random.key(seed)
    key_route, key_head, key_noise, key_row, key_gain = jax.random.split(root_key, 5)
    labels, loss_mask = draw_targets(key_route)
    w_f32 = jax.random.normal(key_head, (D_MODEL, VOCAB_SIZE), jnp.float32) * (LOGIT_STD * D_MODEL ** -0.5)
    label_dirs = jnp.moveaxis(jnp.take(w_f32, labels, axis=1), 0, -1) * (D_MODEL ** 0.5 / LOGIT_STD)
    noise = jax.random.normal(key_noise, (BATCH_SIZE, SEQ_LEN, D_MODEL), jnp.float32)
    row_scale = jax.random.uniform(key_row, (BATCH_SIZE, SEQ_LEN, 1), jnp.float32, 0.5, 2.0)
    hidden = (row_scale * (noise + LABEL_PULL * D_MODEL ** -0.5 * label_dirs)).astype(jnp.bfloat16)
    norm_gain = 1.0 + 0.4 * jax.random.normal(key_gain, (D_MODEL,), jnp.float32)
    return {'hidden': hidden, 'labels': labels, 'loss_mask': loss_mask, 'norm_gain': norm_gain, 'w_head': w_f32.astype(jnp.bfloat16)}


def rms_norm(x_rows, norm_gain):
    inv_rms = lax.rsqrt(jnp.mean(x_rows * x_rows, axis=-1, keepdims=True) + NORM_EPS)
    return x_rows * inv_rms * norm_gain


def reference(hidden, labels, loss_mask, norm_gain, w_head):
    tokens = BATCH_SIZE * SEQ_LEN
    n_blocks = tokens // SEQ_DEV
    x_rows = hidden.reshape(tokens, D_MODEL).astype(jnp.float32)
    norm_out, norm_vjp = jax.vjp(rms_norm, x_rows, norm_gain)
    hn_rows = norm_out.astype(jnp.bfloat16)
    hn_cols = hn_rows.T
    label_ids = labels.reshape(tokens)
    tok_weight = loss_mask.reshape(tokens).astype(jnp.float32)
    kept_count = jnp.sum(tok_weight)

    def token_stats(blk_pair):
        hn_blk, lab_blk = blk_pair
        logits = jnp.dot(hn_blk, w_head, preferred_element_type=jnp.float32)
        row_max = jnp.max(logits, axis=-1)
        blk_norm = row_max + jnp.log(jnp.sum(jnp.exp(logits - row_max[:, None]), axis=-1))
        blk_label = jnp.take_along_axis(logits, lab_blk[:, None], axis=-1)[:, 0]
        return blk_norm, blk_label

    log_norm, label_logit = lax.map(token_stats, (hn_rows.reshape(n_blocks, SEQ_DEV, D_MODEL), label_ids.reshape(n_blocks, SEQ_DEV)))
    log_norm = log_norm.reshape(tokens)
    label_logit = label_logit.reshape(tokens)
    mean_loss = jnp.sum(tok_weight * (log_norm - label_logit)) / kept_count
    tok_scale = tok_weight / kept_count
    w_blocks = jnp.transpose(w_head.reshape(D_MODEL, SHARDS, VSHARD), (1, 0, 2))

    def shard_step(d_norm, shard_in):
        w_blk, shard_idx = shard_in
        logits = jnp.dot(hn_rows, w_blk, preferred_element_type=jnp.float32)
        col_ids = shard_idx * VSHARD + jnp.arange(VSHARD)
        is_label = (label_ids[:, None] == col_ids[None, :]).astype(jnp.float32)
        d_logits = ((jnp.exp(logits - log_norm[:, None]) - is_label) * tok_scale[:, None]).astype(jnp.bfloat16)
        d_blk = jnp.dot(hn_cols, d_logits, preferred_element_type=jnp.float32).astype(jnp.bfloat16)
        dhn_part = jnp.dot(d_logits, w_blk.T, preferred_element_type=jnp.float32).astype(jnp.bfloat16)
        return d_norm + dhn_part.astype(jnp.float32), d_blk

    d_norm, d_blocks = lax.scan(shard_step, jnp.zeros((tokens, D_MODEL), jnp.float32), (w_blocks, jnp.arange(SHARDS)))
    d_head = jnp.transpose(d_blocks, (1, 0, 2)).reshape(D_MODEL, VOCAB_SIZE)
    d_x, d_gain = norm_vjp(d_norm)
    d_hidden = d_x.astype(jnp.bfloat16).reshape(BATCH_SIZE, SEQ_LEN, D_MODEL)
    return mean_loss, d_hidden, d_head, d_gain
```

```python
import jax
import jax.numpy as jnp
from jax import lax
from jax.sharding import PartitionSpec as P

NORM_EPS = 1e-6


def rms_norm(x_rows, norm_gain):
    inv_rms = lax.rsqrt(jnp.mean(x_rows * x_rows, axis=-1, keepdims=True) + NORM_EPS)
    return x_rows * inv_rms * norm_gain


def solution(mesh):
    n_shards = mesh.shape['tp']

    def device_step(hidden, labels, loss_mask, norm_gain, w_head):
        batch_size, seq_loc, model_width = hidden.shape
        v_loc = w_head.shape[1]
        f32 = jnp.float32
        targets = lax.all_gather(jnp.stack([labels, loss_mask]), 'tp', axis=2, tiled=True)
        label_all, mask_all = targets[0], targets[1]
        tok_weight = mask_all.astype(f32)
        kept_count = jnp.sum(tok_weight)
        tok_scale = tok_weight / kept_count
        col_start = lax.axis_index('tp') * v_loc
        loc_label = label_all - col_start

        hn = []
        for b in range(batch_size):
            norm_b = rms_norm(hidden[b].astype(f32), norm_gain).astype(jnp.bfloat16)
            hn.append(lax.all_gather(norm_b, 'tp', axis=0, tiled=True))

        col_ids = lax.broadcasted_iota(jnp.int32, (1, v_loc), 1)
        logits, maxes, sums, picked = [], [], [], []
        for b in range(batch_size):
            z = jnp.dot(hn[b], w_head, preferred_element_type=f32)
            m = jnp.max(z, axis=-1)
            logits.append(z)
            maxes.append(m)
            sums.append(jnp.sum(jnp.exp(z - m[:, None]), axis=-1))
            picked.append(jnp.sum(jnp.where(col_ids == loc_label[b][:, None], z, 0.0), axis=-1))
        stats = lax.all_gather(jnp.stack([jnp.stack(maxes), jnp.stack(sums)]), 'tp', axis=0)
        row_max = jnp.max(stats[:, 0], axis=0)
        sum_exp = jnp.sum(stats[:, 1] * jnp.exp(stats[:, 0] - row_max[None]), axis=0)
        log_norm = row_max + jnp.log(sum_exp)
        owned = (loc_label >= 0) & (loc_label < v_loc)
        loss_part = jnp.sum(jnp.where(owned, tok_weight * (log_norm - jnp.stack(picked)), 0.0))

        d_logits, reduced = [], []
        for b in range(batch_size):
            is_label = (col_ids == loc_label[b][:, None]).astype(f32)
            dz = ((jnp.exp(logits[b] - log_norm[b][:, None]) - is_label) * tok_scale[b][:, None]).astype(jnp.bfloat16)
            d_logits.append(dz)
            part = lax.dot_general(dz, w_head, (((1,), (1,)), ((), ())), preferred_element_type=f32)
            part = lax.reduce_precision(part, 8, 7)
            reduced.append(lax.psum_scatter(part, 'tp', scatter_dimension=0, tiled=True))
        d_head = jnp.zeros((), f32)
        for b in range(batch_size):
            d_head = d_head + lax.dot_general(hn[b], d_logits[b], (((0,), (0,)), ((), ())), preferred_element_type=f32)
        d_head = d_head.astype(jnp.bfloat16)

        d_x, d_gain = [], jnp.zeros((model_width,), f32)
        for b in range(batch_size):
            _, norm_vjp = jax.vjp(rms_norm, hidden[b].astype(f32), norm_gain)
            d_x_b, d_gain_b = norm_vjp(reduced[b])
            d_x.append(d_x_b.astype(jnp.bfloat16))
            d_gain = d_gain + d_gain_b
        tail = lax.psum(jnp.concatenate([d_gain, jnp.full((128,), loss_part / 128.0)]), 'tp')
        mean_loss = jnp.sum(tail[model_width:]) / kept_count
        return mean_loss, jnp.stack(d_x), d_head, tail[:model_width]

    return jax.shard_map(device_step, mesh=mesh, in_specs=(P(None, 'tp', None), P(None, 'tp'), P(None, 'tp'), P(), P(None, 'tp')), out_specs=(P(), P(None, 'tp', None), P(None, 'tp'), P()), check_vma=False)
```

```python
import jax
import jax.numpy as jnp
from jax import lax
from jax.sharding import PartitionSpec as P

NORM_EPS = 1e-6


def rms_norm(x_rows, norm_gain):
    inv_rms = lax.rsqrt(jnp.mean(x_rows * x_rows, axis=-1, keepdims=True) + NORM_EPS)
    return x_rows * inv_rms * norm_gain


def solution(mesh):
    n_shards = mesh.shape['tp']

    def device_step(hidden, labels, loss_mask, norm_gain, w_head):
        batch_size, seq_loc, model_width = hidden.shape
        v_loc = w_head.shape[1]
        f32 = jnp.float32
        lead = seq_loc // 4
        chunks = [(0, 0, lead), (0, lead, seq_loc)] + [(b, 0, seq_loc) for b in range(1, batch_size)]

        x_loc = [hidden[b, lo:hi].astype(f32) for b, lo, hi in chunks]
        hn = []
        for x in x_loc:
            hn.append(lax.all_gather(rms_norm(x, norm_gain).astype(jnp.bfloat16), 'tp', axis=0, tiled=True))

        targets = lax.all_gather(jnp.stack([labels, loss_mask]), 'tp', axis=0)
        col_start = lax.axis_index('tp') * v_loc
        loc_label_all = targets[:, 0] - col_start
        tok_weight_all = targets[:, 1].astype(f32)
        kept_count = jnp.sum(tok_weight_all)
        col_ids = lax.broadcasted_iota(jnp.int32, (1, v_loc), 1)

        loss_part = jnp.zeros((), f32)
        d_logits, reduced = [], []
        part = None
        for i, (b, lo, hi) in enumerate(chunks):
            loc_label = loc_label_all[:, b, lo:hi].reshape(-1)
            tok_weight = tok_weight_all[:, b, lo:hi].reshape(-1)
            h = hn[i]
            if part is not None:
                h, _ = lax.optimization_barrier((h, part))
            z = jnp.dot(h, w_head, preferred_element_type=f32)
            m = jnp.max(z, axis=-1)
            s = jnp.sum(jnp.exp(z - m[:, None]), axis=-1)
            picked = jnp.sum(jnp.where(col_ids == loc_label[:, None], z, 0.0), axis=-1)
            stats = lax.all_gather(jnp.stack([m, s]), 'tp', axis=0)
            row_max = jnp.max(stats[:, 0], axis=0)
            log_norm = row_max + jnp.log(jnp.sum(stats[:, 1] * jnp.exp(stats[:, 0] - row_max[None]), axis=0))
            owned = (loc_label >= 0) & (loc_label < v_loc)
            loss_part = loss_part + jnp.sum(jnp.where(owned, tok_weight * (log_norm - picked), 0.0))
            is_label = (col_ids == loc_label[:, None]).astype(f32)
            dz = ((jnp.exp(z - log_norm[:, None]) - is_label) * (tok_weight / kept_count)[:, None]).astype(jnp.bfloat16)
            dz = lax.optimization_barrier(dz)
            d_logits.append(dz)
            part = lax.dot_general(dz, w_head, (((1,), (1,)), ((), ())), preferred_element_type=f32)
            part = lax.reduce_precision(part, 8, 7)
            reduced.append(lax.psum_scatter(part, 'tp', scatter_dimension=0, tiled=True))
        hn_late, dz_late, _ = lax.optimization_barrier((hn, d_logits, part))
        d_head = jnp.zeros((), f32)
        for h, dz in zip(hn_late, dz_late):
            d_head = d_head + lax.dot_general(h, dz, (((0,), (0,)), ((), ())), preferred_element_type=f32)
        d_head = d_head.astype(jnp.bfloat16)

        d_x, d_gain = [], jnp.zeros((model_width,), f32)
        for x, d_norm in zip(x_loc, reduced):
            _, norm_vjp = jax.vjp(rms_norm, x, norm_gain)
            d_x_i, d_gain_i = norm_vjp(d_norm)
            d_x.append(d_x_i.astype(jnp.bfloat16))
            d_gain = d_gain + d_gain_i
        tail = lax.psum(jnp.concatenate([d_gain, jnp.full((128,), loss_part / 128.0)]), 'tp')
        mean_loss = jnp.sum(tail[model_width:]) / kept_count
        d_hidden = jnp.zeros(hidden.shape, jnp.bfloat16)
        for (b, lo, hi), d_x_i in zip(chunks, d_x):
            d_hidden = lax.dynamic_update_slice(d_hidden, d_x_i[None], (b, lo, 0))
        return mean_loss, d_hidden, d_head, tail[:model_width]

    return jax.shard_map(device_step, mesh=mesh, in_specs=(P(None, 'tp', None), P(None, 'tp'), P(None, 'tp'), P(), P(None, 'tp')), out_specs=(P(), P(None, 'tp', None), P(None, 'tp'), P()), check_vma=False)
```

```python
import jax
import jax.numpy as jnp
from jax import lax
from jax.sharding import PartitionSpec as P

NORM_EPS = 1e-6


def rms_norm(x_rows, norm_gain):
    inv_rms = lax.rsqrt(jnp.mean(x_rows * x_rows, axis=-1, keepdims=True) + NORM_EPS)
    return x_rows * inv_rms * norm_gain


def solution(mesh):
    n_shards = mesh.shape['tp']

    def device_step(hidden, labels, loss_mask, norm_gain, w_head):
        batch_size, seq_loc, model_width = hidden.shape
        v_loc = w_head.shape[1]
        f32 = jnp.float32
        lead = seq_loc // 4
        chunks = [(0, 0, lead), (0, lead, seq_loc)] + [(b, 0, seq_loc) for b in range(1, batch_size)]

        x_loc = [hidden[b, lo:hi].astype(f32) for b, lo, hi in chunks]
        hn = []
        for x in x_loc:
            hn.append(lax.all_gather(rms_norm(x, norm_gain).astype(jnp.bfloat16), 'tp', axis=0, tiled=True))

        targets = lax.all_gather(jnp.stack([labels, loss_mask]), 'tp', axis=0)
        col_start = lax.axis_index('tp') * v_loc
        loc_label_all = targets[:, 0] - col_start
        tok_weight_all = targets[:, 1].astype(f32)
        kept_count = jnp.sum(tok_weight_all)
        col_ids = lax.broadcasted_iota(jnp.int32, (1, v_loc), 1)

        loss_part = jnp.zeros((), f32)
        d_logits, reduced = [], []
        part = None
        for i, (b, lo, hi) in enumerate(chunks):
            loc_label = loc_label_all[:, b, lo:hi].reshape(-1)
            tok_weight = tok_weight_all[:, b, lo:hi].reshape(-1)
            h = hn[i]
            if part is not None:
                h, _ = lax.optimization_barrier((h, part))
            z = jnp.dot(h, w_head, preferred_element_type=f32)
            m = jnp.max(z, axis=-1)
            s = jnp.sum(jnp.exp(z - m[:, None]), axis=-1)
            picked = jnp.sum(jnp.where(col_ids == loc_label[:, None], z, 0.0), axis=-1)
            stats = lax.all_gather(jnp.stack([m, s]), 'tp', axis=0)
            row_max = jnp.max(stats[:, 0], axis=0)
            log_norm = row_max + jnp.log(jnp.sum(stats[:, 1] * jnp.exp(stats[:, 0] - row_max[None]), axis=0))
            owned = (loc_label >= 0) & (loc_label < v_loc)
            loss_part = loss_part + jnp.sum(jnp.where(owned, tok_weight * (log_norm - picked), 0.0))
            is_label = (col_ids == loc_label[:, None]).astype(f32)
            dz = ((jnp.exp(z - log_norm[:, None]) - is_label) * (tok_weight / kept_count)[:, None]).astype(jnp.bfloat16)
            dz = lax.optimization_barrier(dz)
            d_logits.append(dz)
            part = lax.dot_general(dz, w_head, (((1,), (1,)), ((), ())), preferred_element_type=f32)
            part = lax.reduce_precision(part, 8, 7)
            reduced.append(lax.psum_scatter(part, 'tp', scatter_dimension=0, tiled=True))
        hn_late, dz_late, _ = lax.optimization_barrier((hn, d_logits, part))
        d_head = None
        for h, dz in zip(hn_late, dz_late):
            term = lax.dot_general(h, dz, (((0,), (0,)), ((), ())), preferred_element_type=f32)
            d_head = term if d_head is None else lax.optimization_barrier(d_head) + term
        d_head = d_head.astype(jnp.bfloat16)

        d_x, d_gain = [], jnp.zeros((model_width,), f32)
        for x, d_norm in zip(x_loc, reduced):
            _, norm_vjp = jax.vjp(rms_norm, x, norm_gain)
            d_x_i, d_gain_i = norm_vjp(d_norm)
            d_x.append(d_x_i.astype(jnp.bfloat16))
            d_gain = d_gain + d_gain_i
        tail = jnp.sum(lax.all_gather(jnp.concatenate([d_gain, jnp.full((128,), loss_part / 128.0)]), 'tp', axis=0), axis=0)
        mean_loss = jnp.sum(tail[model_width:]) / kept_count
        d_hidden = jnp.zeros(hidden.shape, jnp.bfloat16)
        for (b, lo, hi), d_x_i in zip(chunks, d_x):
            d_hidden = lax.dynamic_update_slice(d_hidden, d_x_i[None], (b, lo, 0))
        return mean_loss, d_hidden, d_head, tail[:model_width]

    return jax.shard_map(device_step, mesh=mesh, in_specs=(P(None, 'tp', None), P(None, 'tp'), P(None, 'tp'), P(), P(None, 'tp')), out_specs=(P(), P(None, 'tp', None), P(None, 'tp'), P()), check_vma=False)
```
